32 devices in a mesh: dp: 8 (over z, core), seq: 4 (over y, x).
Axes of the slice: x: 2, y: 2, z: 4, core: 2. Of those that a mesh axis runs over, the one named last changes fastest.
Arguments:
- layer_in: bfloat16 [8, 512, 2560], P('dp', 'seq'), may hold values from -6 to 6
- scan_in: bfloat16 [8, 512, 2560], P('dp', 'seq'), may hold values from -6 to 6
- step_size: float32 [8, 512, 40], P('dp', 'seq'), may hold values from 0.0024 to 0.041
- b_weight: bfloat16 [2560, 64], replicated, may hold values from -0.125 to 0.125
- c_weight: bfloat16 [2560, 64], replicated, may hold values from -0.125 to 0.125
- decay_rate: float32 [40], replicated, may hold values from 0.0005 to 10
- skip_gain: float32 [40], replicated, may hold values from 0.25 to 1.75
- out_grad: bfloat16 [8, 512, 2560], P('dp', 'seq'), may hold values from -6 to 6
- doc_lengths: int32 [8, 4], P('dp'), may hold values from 1 to 256, 512 in all within a row
- block_order: int32 [8, 4], P('dp'), may hold values from 0 to 3, each once within a row
Outputs:
- scan_out: bfloat16 [8, 512, 2560], P('dp', 'seq')
- b_weight_grad: float32 [2560, 64], replicated
- c_weight_grad: float32 [2560, 64], replicated
The draws below stay inside these ranges and needn't reach their ends.
Inputs may be any that keep to these rules, and one draw needn't show every extreme that they name: `block_order`: each row holds 0 to 3 once each. `doc_lengths`: each row sums to 512; its longest document has 256 tokens.
All inputs are finite; a program needn't handle non-finite values.
Results may differ from the reference program's by a relative error of at most 0.0055.
Values sent between devices are 32-bit elements.
A program may use at most 128 MiB of HBM per device.

```python
import math
import jax
import jax.numpy as jnp
import numpy as np
from jax import lax

D = 2560
INNER = 2560
STATE = 64
HEAD_DIM = 64
HEADS = 40
T_DEV = 128
DOCS = 4
SEQLEN = 512
MOSTLEN = 256
GROUPS = 8
N_SEQ = 4


def draw_step_size(key, part):
    key = jax.random.fold_in(key, 11)
    jitter_key, level_key = jax.random.split(key)
    jitter = jax.random.uniform(jitter_key, (GROUPS, SEQLEN // T_DEV, T_DEV, HEADS), jnp.float32, -0.7, 0.7)
    block_level = jax.random.uniform(level_key, (GROUPS, SEQLEN // T_DEV, 1, HEADS), jnp.float32, -0.7, 0.7)
    return (0.01 * jnp.exp(jitter + block_level)).reshape(GROUPS, SEQLEN, HEADS)


def draw_decay_rate(key, part):
    key = jax.random.fold_in(key, 23)
    pick_key, slow_key, fast_key = jax.random.split(key, 3)
    slow_share = 0.5
    slow_mask = jax.random.uniform(pick_key, (HEADS,), jnp.float32) < slow_share
    slow_rate = jnp.exp(jax.random.uniform(slow_key, (HEADS,), jnp.float32, math.log(0.0005), math.log(0.005)))
    fast_rate = jnp.exp(jax.random.uniform(fast_key, (HEADS,), jnp.float32, math.log(2.0), math.log(10.0)))
    return jnp.where(slow_mask, slow_rate, fast_rate)


def shard_levels(own_key, shape, pieces, smallest, high):
    def one(position, shards_of):
        draws = jax.random.uniform(jax.random.fold_in(jax.random.fold_in(own_key, 6), position), (shards_of,), jnp.float32, smallest / len(pieces), high / len(pieces))
        return jnp.repeat(jnp.exp(draws), shape[position] // shards_of).reshape((-1,) + (1,) * (len(shape) - position - 1))

    gain = one(*pieces[0])
    for cut in pieces[1:]:
        gain = gain * one(*cut)
    return gain


def split_up(number_of, total, reach, lean):
    portions = [(1 << 20) // math.isqrt(grade ** lean) + 1 for grade in range(2, number_of + 1)]
    spare, counts = total - reach - (number_of - 1), [1] * (number_of - 1)
    while spare > 0:
        free = [i for i in range(number_of - 1) if counts[i] < reach]
        whole, budget = sum([portions[i] for i in free]), spare
        for i in free:
            more = min(reach - counts[i], max(1, budget * portions[i] // whole), spare)
            counts[i] = counts[i] + more
            spare = spare - more
    return np.array([reach] + counts)


def ragged_sizes(rng, count, total, most, slope):
    if count == 2:
        one = jax.random.randint(rng, (), max(1, total - most), min(most, total - 1) + 1)
        return jnp.stack([one, total - one])
    tallies = jnp.asarray(split_up(count, total, most, slope), jnp.int32)
    couples = (count - 1) // 2
    donor, receiver = tallies[1:1 + 2 * couples:2], tallies[2:2 + 2 * couples:2]
    slack = jnp.minimum(donor - 1, most - receiver)
    shifted = jax.random.randint(jax.random.fold_in(rng, 1), (couples,), 0, 1 << 20) % (slack + 1)
    tallies = tallies.at[1:1 + 2 * couples:2].set(donor - shifted).at[2:2 + 2 * couples:2].set(receiver + shifted)
    return tallies[jax.random.permutation(jax.random.fold_in(rng, 2), count)]


def normal_values(key, extent, scale, reach, cuts=(), kind=jnp.bfloat16):
    level = shard_levels(key, extent, cuts, -0.22, 0.18) if cuts else 1.0
    values = jax.random.normal(key, extent, jnp.float32) * scale * level
    return jnp.minimum(jnp.maximum(values, -reach), reach).astype(kind)


def setup_inputs(seed: int = 0) -> dict:
    arg_keys = jax.random.split(jax.random.key(seed), 11)
    return {
        "layer_in": normal_values(arg_keys[0], (GROUPS, SEQLEN, D), 1.0, 6.0, ((0, 8), (1, 4))),
        "scan_in": normal_values(arg_keys[1], (GROUPS, SEQLEN, INNER), 1.0, 6.0, ((0, 8), (1, 4))),
        "step_size": draw_step_size(jax.random.fold_in(arg_keys[10], 71), 0),
        "b_weight": normal_values(arg_keys[3], (D, STATE), D ** -0.5, 0.125),
        "c_weight": normal_values(arg_keys[4], (D, STATE), D ** -0.5, 0.125),
        "decay_rate": draw_decay_rate(jax.random.fold_in(arg_keys[10], 71), 0),
        "skip_gain": jnp.clip(1.0 + 0.15 * jax.random.normal(arg_keys[6], (HEADS,), jnp.float32), 0.25, 1.75),
        "out_grad": normal_values(arg_keys[7], (GROUPS, SEQLEN, INNER), 1.0, 6.0, ((0, 8), (1, 4))),
        "doc_lengths": jax.vmap(lambda own: ragged_sizes(own, DOCS, SEQLEN, MOSTLEN, 2))(jax.random.split(arg_keys[8], GROUPS)).reshape((GROUPS, DOCS)).astype(jnp.int32),
        "block_order": jax.vmap(lambda own: jax.random.permutation(own, N_SEQ))(jax.random.split(arg_keys[9], GROUPS)).reshape((GROUPS, N_SEQ)).astype(jnp.int32),
    }


def group_pass(scan_grp, step_grp, grad_grp, lengths, order_row, b_grp, c_grp, decay_rate, skip_gain):
    head_count = decay_rate.shape[0]
    inverse = jnp.zeros((N_SEQ,), jnp.int32).at[order_row].set(jnp.arange(N_SEQ, dtype=jnp.int32))

    def to_sequence(values):
        return values.reshape((N_SEQ, T_DEV) + values.shape[1:])[inverse].reshape((SEQLEN,) + values.shape[1:])

    def to_held(values):
        return values.reshape((N_SEQ, T_DEV) + values.shape[1:])[order_row].reshape((SEQLEN,) + values.shape[1:])

    seq_x = to_sequence(scan_grp).reshape(SEQLEN, head_count, HEAD_DIM)
    seq_grad = to_sequence(grad_grp).reshape(SEQLEN, head_count, HEAD_DIM)
    seq_step = to_sequence(step_grp)
    seq_b = to_sequence(b_grp).astype(jnp.float32)
    seq_c = to_sequence(c_grp).astype(jnp.float32)
    doc_ends = jnp.cumsum(lengths, dtype=jnp.int32)
    doc_starts = doc_ends - lengths
    positions = jnp.arange(SEQLEN, dtype=jnp.int32)
    begins = jnp.any(positions[:, None] == doc_starts[None, :], axis=1)
    decay = jnp.where(begins[:, None], jnp.float32(0.0), jnp.exp(-seq_step * decay_rate[None, :]))

    def forward(state_now, inputs):
        decay_now, step_now, x_row, b_row, c_row, grad_row = inputs
        x_float = x_row.astype(jnp.float32)
        state_now = decay_now[:, None, None] * state_now + (step_now[:, None] * x_float)[:, :, None] * b_row[None, None, :]
        out_row = jnp.sum(state_now * c_row[None, None, :], axis=2) + skip_gain[:, None] * x_float
        dc_row = jnp.sum(state_now * grad_row.astype(jnp.float32)[:, :, None], axis=(0, 1))
        return state_now, (out_row.astype(jnp.bfloat16), dc_row.astype(jnp.bfloat16))

    zero_state = jnp.zeros((head_count, HEAD_DIM, STATE), jnp.float32)
    _, (outs_seq, dc_seq) = lax.scan(forward, zero_state, (decay, seq_step, seq_x, seq_b, seq_c, seq_grad))
    next_decay = jnp.concatenate([decay[1:], jnp.zeros((1, head_count), jnp.float32)], axis=0)

    def backward(adjoint, inputs):
        decay_next, step_now, x_row, c_row, grad_row = inputs
        adjoint = decay_next[:, None, None] * adjoint + grad_row.astype(jnp.float32)[:, :, None] * c_row[None, None, :]
        db_row = jnp.sum(adjoint * (step_now[:, None] * x_row.astype(jnp.float32))[:, :, None], axis=(0, 1))
        return adjoint, db_row.astype(jnp.bfloat16)

    _, db_seq = lax.scan(backward, zero_state, (next_decay, seq_step, seq_x, seq_c, seq_grad), reverse=True)
    return to_held(outs_seq.reshape(SEQLEN, head_count * HEAD_DIM)), to_held(dc_seq), to_held(db_seq)


def reference(layer_in, scan_in, step_size, b_weight, c_weight, decay_rate, skip_gain, out_grad, doc_lengths, block_order):
    group_count = layer_in.shape[0]
    token_rows = layer_in.reshape(-1, D)
    b_all = jnp.dot(token_rows, b_weight, preferred_element_type=jnp.float32).astype(jnp.bfloat16).reshape(group_count, SEQLEN, STATE)
    c_all = jnp.dot(token_rows, c_weight, preferred_element_type=jnp.float32).astype(jnp.bfloat16).reshape(group_count, SEQLEN, STATE)

    def run_group(inputs):
        return group_pass(*inputs, decay_rate, skip_gain)

    outs_all, dc_all, db_all = lax.map(run_group, (scan_in, step_size, out_grad, doc_lengths, block_order, b_all, c_all))
    scale = 1.0 / (group_count * SEQLEN)
    b_grad = jnp.dot(token_rows.T, db_all.reshape(-1, STATE), preferred_element_type=jnp.float32) * scale
    c_grad = jnp.dot(token_rows.T, dc_all.reshape(-1, STATE), preferred_element_type=jnp.float32) * scale
    return outs_all, b_grad, c_grad
```

```python
import functools
import math

import jax
import jax.numpy as jnp
from jax import lax
from jax.experimental import pallas as pl
from jax.experimental.pallas import tpu as pltpu
from jax.sharding import PartitionSpec as P

MESH = pl.DeviceIdType.MESH
F32 = jnp.float32
BF16 = jnp.bfloat16


def dot(a, b):
    return jnp.dot(a, b, preferred_element_type=F32)


def dot_nt(a, b):
    return lax.dot_general(a, b, (((1,), (1,)), ((), ())), preferred_element_type=F32)


def dot_tn(a, b):
    return lax.dot_general(a, b, (((0,), (0,)), ((), ())), preferred_element_type=F32)


def spread(values, expander):
    high = values.astype(BF16)
    low = (values - high.astype(F32)).astype(BF16)
    return dot(high, expander) + dot(low, expander)


def plan(n_dp, n_seq):
    cores = 2 if n_dp % 2 == 0 else 1
    nz = n_dp // cores
    nx = math.isqrt(n_seq)
    while n_seq % nx:
        nx -= 1
    return cores, nz, nx, n_seq // nx


def kernel(
    n_dp,
    n_seq,
    depth,
    tok_ref,
    x_ref,
    step_ref,
    bw_ref,
    cw_ref,
    rate_ref,
    skip_ref,
    g_ref,
    len_ref,
    order_ref,
    y_ref,
    grad_ref,
    u_buf,
    v_buf,
    ec_buf,
    yin_buf,
    t_send,
    t_recv,
    tot_send,
    tot_recv,
    part,
    whole,
    rs0,
    rs1,
    rs2,
    rs3,
    t_ssem,
    t_rsem,
    tot_ssem,
    tot_rsem,
    rs_ssem,
    rs_rsem,
    ag_ssem,
    ag_rsem,
):
    dp = lax.axis_index("dp")
    me = lax.axis_index("seq")
    cores, nz, nx, ny = plan(n_dp, n_seq)
    core, z = dp % cores, dp // cores
    px, py = me % nx, me // nx
    rows, inner = x_ref.shape[1], x_ref.shape[2]
    heads = step_ref.shape[2]
    width = inner // heads
    states = bw_ref.shape[1]
    cut = 512 if inner % 512 == 0 else inner

    def along_x(k):
        return (dp, py * nx + (px + k) % nx)

    def along_y(k):
        return (dp, ((py + k) % ny) * nx + px)

    def mixed(first, second, k):
        a, b = first(k)[1], second(k)[1]
        return (dp, (1 - core) * a + core * b)

    def to_core(k):
        return (z * cores + (core + k) % cores, me)

    def to_z(k):
        return (((z + k) % nz) * cores + core, me)

    if nx == ny and cores == 2:
        pos1, pos2 = (1 - core) * px + core * py, (1 - core) * py + core * px
        stage1 = functools.partial(mixed, along_x, along_y)
        stage2 = functools.partial(mixed, along_y, along_x)
    else:
        pos1, pos2, stage1, stage2 = px, py, along_x, along_y
    stages = (
        (cores, core, to_core, rs0),
        (nx, pos1, stage1, rs1),
        (ny, pos2, stage2, rs2),
        (nz, z, to_z, rs3),
    )

    barrier = pltpu.get_barrier_semaphore()
    greeted = 0
    for k in range(1, n_seq):
        pl.semaphore_signal(
            barrier, inc=1, device_id=(dp, (me + k) % n_seq), device_id_type=MESH
        )
        greeted += 1
    for count, _, peer, _ in (stages[0], stages[3]):
        for k in range(1, count):
            pl.semaphore_signal(barrier, inc=1, device_id=peer(k), device_id_type=MESH)
            greeted += 1

    mine = order_ref[0, me]
    first = mine * rows
    starts = []
    running = jnp.int32(0)
    for j in range(len_ref.shape[1]):
        starts.append(running)
        running = running + len_ref[0, j]

    def segment_of(place):
        total = jnp.zeros_like(place)
        for start in starts:
            total = total + jnp.where(place >= start, 1, 0)
        return total

    seg_col = segment_of(first + lax.broadcasted_iota(jnp.int32, (rows, 1), 0))
    seg_row = segment_of(first + lax.broadcasted_iota(jnp.int32, (1, rows), 1))
    begun = jnp.int32(0)
    first_seg = jnp.int32(0)
    last_seg = jnp.int32(0)
    for start in starts:
        begun = begun + jnp.where(start == first, 1, 0)
        first_seg = first_seg + jnp.where(start <= first, 1, 0)
        last_seg = last_seg + jnp.where(start <= first + rows - 1, 1, 0)
    link_seg = first_seg - 1000 * begun
    linked = jnp.where(seg_col == link_seg, F32(1.0), F32(0.0))
    in_last = jnp.where(seg_col == last_seg, F32(1.0), F32(0.0))
    through = jnp.where(
        jnp.full((1, heads), link_seg, jnp.int32) == last_seg, F32(1.0), F32(0.0)
    )

    spot_t = lax.broadcasted_iota(jnp.int32, (rows, rows), 0)
    spot_s = lax.broadcasted_iota(jnp.int32, (rows, rows), 1)
    lower = spot_t >= spot_s
    causal = lower & (seg_col == seg_row)
    steps = step_ref[0]
    cumlog = lax.dot_general(
        jnp.where(lower, F32(1.0), F32(0.0)),
        -(steps * rate_ref[...]),
        (((1,), (0,)), ((), ())),
        precision=lax.Precision.HIGHEST,
        preferred_element_type=F32,
    )
    grown = jnp.exp(cumlog)
    shrunk = jnp.exp(-cumlog) * steps
    total = grown[rows - 1 : rows, :] * through
    tot_send[...] = jnp.zeros_like(tot_send)
    tot_send[:, :heads] = jnp.broadcast_to(total, (tot_send.shape[0], heads))

    tokens = tok_ref[0]
    b_mat = dot(tokens, bw_ref[...]).astype(BF16)
    c_mat = dot(tokens, cw_ref[...]).astype(BF16)
    b_float, c_float = b_mat.astype(F32), c_mat.astype(F32)
    b_last = jnp.transpose(b_float * in_last).astype(BF16)
    c_linked = c_float * linked
    c_turned = jnp.transpose(c_linked).astype(BF16)
    c_linked = c_linked.astype(BF16)

    def expander(at):
        head = lax.broadcasted_iota(jnp.int32, (heads, cut), 0)
        lane = lax.broadcasted_iota(jnp.int32, (heads, cut), 1) + at
        inside = (lane >= head * width) & (lane < head * width + width)
        return jnp.where(inside, F32(1.0), F32(0.0)).astype(BF16)

    sent_orders = [order_ref[0, (me + k) % n_seq] for k in range(1, n_seq)]
    got_orders = [order_ref[0, (me + n_seq - k) % n_seq] for k in range(1, n_seq)]
    for at in range(0, inner, cut):
        lanes = slice(at, at + cut)
        spreader = expander(at)
        grown_x = spread(grown, spreader)
        ec_buf[:, lanes] = grown_x
        u_part = (x_ref[0, :, lanes].astype(F32) * spread(shrunk, spreader)).astype(BF16)
        v_part = (g_ref[0, :, lanes].astype(F32) * grown_x).astype(BF16)
        u_buf[:, lanes] = u_part
        v_buf[:, lanes] = v_part
        state = dot(b_last, u_part) * grown_x[rows - 1 : rows, :]
        adjoint = dot(c_turned, v_part)
        for k in range(1, n_seq):
            later = jnp.full(state.shape, sent_orders[k - 1], jnp.int32) > mine
            t_send[k - 1, :, lanes] = jnp.where(later, state, adjoint)

    pl.semaphore_wait(barrier, greeted)
    sends = []
    for k in range(1, n_seq):
        target = (dp, (me + k) % n_seq)
        for source, landing, ssem, rsem in (
            (tot_send, tot_recv.at[k - 1], tot_ssem, tot_rsem),
            (t_send.at[k - 1], t_recv.at[k - 1], t_ssem, t_rsem),
        ):
            copy = pltpu.make_async_remote_copy(
                src_ref=source,
                dst_ref=landing,
                send_sem=ssem.at[k - 1],
                recv_sem=rsem.at[k - 1],
                device_id=target,
                device_id_type=MESH,
            )
            copy.start()
            sends.append(copy)

    scores = jnp.where(causal, dot_nt(c_mat, b_mat), F32(0.0)).astype(BF16)
    mixing = jnp.zeros((rows, rows), F32)
    for at in range(0, inner, cut):
        lanes = slice(at, at + cut)
        u_part = u_buf[:, lanes]
        yin_buf[:, lanes] = dot(scores, u_part)
        mixing = mixing + dot_nt(v_buf[:, lanes], u_part)
    mixing = jnp.where(causal, mixing, F32(0.0))
    grad_c = dot(mixing.astype(BF16), b_mat)
    grad_b = dot(jnp.transpose(mixing).astype(BF16), c_mat)

    for copy in sends:
        copy.wait()

    weights = []
    for k in range(n_seq - 1):
        weight = jnp.ones((8, heads), F32)
        own = jnp.full((8, heads), got_orders[k], jnp.int32)
        low, high = jnp.minimum(own, mine), jnp.maximum(own, mine)
        for other in range(n_seq - 1):
            if other != k:
                inside = (low < got_orders[other]) & (got_orders[other] < high)
                weight = weight * jnp.where(inside, tot_recv[other, :, :heads], F32(1.0))
        weights.append(weight)
    skips = jnp.broadcast_to(skip_ref[...], (8, heads))
    cross_c = jnp.zeros((rows, states), F32)
    cross_b = jnp.zeros((rows, states), F32)
    for at in range(0, inner, cut):
        lanes = slice(at, at + cut)
        spreader = expander(at)
        incoming = jnp.zeros((states, cut), F32)
        returning = jnp.zeros((states, cut), F32)
        for k in range(n_seq - 1):
            term = t_recv[k, :, lanes] * spread(weights[k], spreader)[:1, :]
            earlier = jnp.full(term.shape, got_orders[k], jnp.int32) < mine
            incoming = incoming + jnp.where(earlier, term, F32(0.0))
            returning = returning + jnp.where(earlier, F32(0.0), term)
        grown_x = ec_buf[:, lanes]
        incoming = incoming.astype(BF16)
        returning = (returning * grown_x[rows - 1 : rows, :]).astype(BF16)
        y_part = grown_x * (yin_buf[:, lanes] + dot(c_linked, incoming))
        y_part = y_part + spread(skips, spreader)[:1, :] * x_ref[0, :, lanes].astype(F32)
        y_ref[0, :, lanes] = y_part.astype(BF16)
        cross_c = cross_c + dot_nt(v_buf[:, lanes], incoming)
        cross_b = cross_b + dot_nt(u_buf[:, lanes], returning)
    grad_c = (grad_c + cross_c * linked).astype(BF16)
    grad_b = (grad_b + cross_b * in_last).astype(BF16)

    part[:depth, :states] = dot_tn(tokens, grad_b)
    part[:depth, states:] = dot_tn(tokens, grad_c)
    if part.shape[0] > depth:
        part[depth:, :] = jnp.zeros((part.shape[0] - depth, part.shape[1]), F32)

    base = jnp.int32(0)
    extent = part.shape[0]
    owned = []
    used = 0
    for count, place, peer, landing in stages:
        extent = extent // count
        copies = []
        for k in range(1, count):
            theirs = pl.multiple_of(base + ((place + k) % count) * extent, 8)
            copy = pltpu.make_async_remote_copy(
                src_ref=part.at[pl.ds(theirs, extent)],
                dst_ref=landing.at[k - 1],
                send_sem=rs_ssem.at[used],
                recv_sem=rs_rsem.at[used],
                device_id=peer(k),
                device_id_type=MESH,
            )
            copy.start()
            copies.append(copy)
            used += 1
        base = pl.multiple_of(base + place * extent, 8)
        owned.append((base, extent))
        summed = part[pl.ds(base, extent), :]
        for k, copy in enumerate(copies):
            copy.wait()
            summed = summed + landing[k]
        part[pl.ds(base, extent), :] = summed
    whole[pl.ds(base, extent), :] = part[pl.ds(base, extent), :]

    used = 0
    for (count, place, peer, _), (at, extent) in zip(stages[::-1], owned[::-1]):
        copies = []
        for k in range(1, count):
            copy = pltpu.make_async_remote_copy(
                src_ref=whole.at[pl.ds(at, extent)],
                dst_ref=whole.at[pl.ds(at, extent)],
                send_sem=ag_ssem.at[used],
                recv_sem=ag_rsem.at[used],
                device_id=peer(k),
                device_id_type=MESH,
            )
            copy.start()
            copies.append(copy)
            used += 1
        for copy in copies:
            copy.wait()
    grad_ref[...] = whole[:depth, :]


def per_device(
    layer_in,
    scan_in,
    step_size,
    b_weight,
    c_weight,
    decay_rate,
    skip_gain,
    out_grad,
    doc_lengths,
    block_order,
):
    n_dp, n_seq = lax.axis_size("dp"), lax.axis_size("seq")
    rows, inner = scan_in.shape[1], scan_in.shape[2]
    depth, states = b_weight.shape
    cores, nz, nx, ny = plan(n_dp, n_seq)
    devices = n_dp * n_seq
    padded = devices * 8 * (-(-depth // (devices * 8)))
    landings = []
    extent = padded
    for count in (cores, nx, ny, nz):
        extent = extent // count
        landings.append(pltpu.VMEM((max(count - 1, 1), extent, 2 * states), F32))
    hops = max(cores + nx + ny + nz - 4, 1)
    links = max(n_seq - 1, 1)
    vmem = pl.BlockSpec(memory_space=pltpu.VMEM)
    smem = pl.BlockSpec(memory_space=pltpu.SMEM)
    dma = pltpu.SemaphoreType.DMA
    scan_out, grads = pl.pallas_call(
        functools.partial(kernel, n_dp, n_seq, depth),
        out_shape=(
            jax.ShapeDtypeStruct((1, rows, inner), BF16),
            jax.ShapeDtypeStruct((depth, 2 * states), F32),
        ),
        in_specs=[vmem] * 8 + [smem] * 2,
        out_specs=(vmem, vmem),
        scratch_shapes=[
            pltpu.VMEM((rows, inner), BF16),
            pltpu.VMEM((rows, inner), BF16),
            pltpu.VMEM((rows, inner), F32),
            pltpu.VMEM((rows, inner), F32),
            pltpu.VMEM((links, states, inner), F32),
            pltpu.VMEM((links, states, inner), F32),
            pltpu.VMEM((8, 128), F32),
            pltpu.VMEM((links, 8, 128), F32),
            pltpu.VMEM((padded, 2 * states), F32),
            pltpu.VMEM((padded, 2 * states), F32),
            *landings,
            dma((links,)),
            dma((links,)),
            dma((links,)),
            dma((links,)),
            dma((hops,)),
            dma((hops,)),
            dma((hops,)),
            dma((hops,)),
        ],
        compiler_params=pltpu.CompilerParams(
            collective_id=0, has_side_effects=True, vmem_limit_bytes=60 * 1024 * 1024
        ),
    )(
        layer_in,
        scan_in,
        step_size,
        b_weight,
        c_weight,
        decay_rate[None, :],
        skip_gain[None, :],
        out_grad,
        doc_lengths,
        block_order,
    )
    scale = 1.0 / (n_dp * n_seq * rows)
    return (scan_out, grads[:, :states] * scale, grads[:, states:] * scale)


def solution(mesh):
    blocks = P("dp", "seq", None)
    in_specs = (blocks, blocks, blocks, P(), P(), P(), P(), blocks, P("dp", None), P("dp", None))
    return jax.shard_map(
        per_device, mesh=mesh, in_specs=in_specs, out_specs=(blocks, P(), P()), check_vma=False
    )
```

```python
import functools
import math

import jax
import jax.numpy as jnp
from jax import lax
from jax.experimental import pallas as pl
from jax.experimental.pallas import tpu as pltpu
from jax.sharding import PartitionSpec as P

MESH = pl.DeviceIdType.MESH
F32 = jnp.float32
BF16 = jnp.bfloat16


def dot(a, b):
    return jnp.dot(a, b, preferred_element_type=F32)


def dot_nt(a, b):
    return lax.dot_general(a, b, (((1,), (1,)), ((), ())), preferred_element_type=F32)


def dot_tn(a, b):
    return lax.dot_general(a, b, (((0,), (0,)), ((), ())), preferred_element_type=F32)


def spread(values, expander):
    high = values.astype(BF16)
    low = (values - high.astype(F32)).astype(BF16)
    return dot(high, expander) + dot(low, expander)


def plan(n_dp, n_seq):
    cores = 2 if n_dp % 2 == 0 else 1
    nz = n_dp // cores
    nx = math.isqrt(n_seq)
    while n_seq % nx:
        nx -= 1
    return cores, nz, nx, n_seq // nx


def kernel(
    n_dp,
    n_seq,
    depth,
    tok_ref,
    x_ref,
    step_ref,
    bw_ref,
    cw_ref,
    rate_ref,
    skip_ref,
    g_ref,
    len_ref,
    order_ref,
    y_ref,
    gb_ref,
    gc_ref,
    u_buf,
    v_buf,
    ec_buf,
    yin_buf,
    in_buf,
    t_send,
    t_recv,
    tot_send,
    tot_recv,
    part,
    whole,
    rs0,
    rs1,
    rs2,
    rs3,
    t_ssem,
    t_rsem,
    tot_ssem,
    tot_rsem,
    rs_ssem,
    rs_rsem,
    ag_ssem,
    ag_rsem,
):
    dp = lax.axis_index("dp")
    me = lax.axis_index("seq")
    cores, nz, nx, ny = plan(n_dp, n_seq)
    core, z = dp % cores, dp // cores
    px, py = me % nx, me // nx
    rows, inner = x_ref.shape[1], x_ref.shape[2]
    heads = step_ref.shape[1]
    width = inner // heads
    states = bw_ref.shape[0]
    lane_cut = 128
    cut = 512 if inner % 512 == 0 else inner

    def along_x(k):
        return (dp, py * nx + (px + k) % nx)

    def along_y(k):
        return (dp, ((py + k) % ny) * nx + px)

    def mixed(first, second, k):
        a, b = first(k)[1], second(k)[1]
        return (dp, (1 - core) * a + core * b)

    def to_core(k):
        return (z * cores + (core + k) % cores, me)

    def to_z(k):
        return (((z + k) % nz) * cores + core, me)

    if nx == ny and cores == 2:
        pos1, pos2 = (1 - core) * px + core * py, (1 - core) * py + core * px
        stage1 = functools.partial(mixed, along_x, along_y)
        stage2 = functools.partial(mixed, along_y, along_x)
    else:
        pos1, pos2, stage1, stage2 = px, py, along_x, along_y
    stages = (
        (cores, core, to_core, rs0),
        (nx, pos1, stage1, rs1),
        (ny, pos2, stage2, rs2),
        (nz, z, to_z, rs3),
    )

    barrier = pltpu.get_barrier_semaphore()
    greeted = 0
    for k in range(1, n_seq):
        pl.semaphore_signal(
            barrier, inc=1, device_id=(dp, (me + k) % n_seq), device_id_type=MESH
        )
        greeted += 1
    for count, _, peer, _ in (stages[0], stages[3]):
        for k in range(1, count):
            pl.semaphore_signal(barrier, inc=1, device_id=peer(k), device_id_type=MESH)
            greeted += 1

    mine = order_ref[0, me]
    first = mine * rows
    starts = []
    running = jnp.int32(0)
    for j in range(len_ref.shape[1]):
        starts.append(running)
        running = running + len_ref[0, j]

    def segment_of(place):
        total = jnp.zeros_like(place)
        for start in starts:
            total = total + jnp.where(place >= start, 1, 0)
        return total

    seg_col = segment_of(first + lax.broadcasted_iota(jnp.int32, (rows, 1), 0))
    seg_row = segment_of(first + lax.broadcasted_iota(jnp.int32, (1, rows), 1))
    begun = jnp.int32(0)
    first_seg = jnp.int32(0)
    last_seg = jnp.int32(0)
    for start in starts:
        begun = begun + jnp.where(start == first, 1, 0)
        first_seg = first_seg + jnp.where(start <= first, 1, 0)
        last_seg = last_seg + jnp.where(start <= first + rows - 1, 1, 0)
    link_seg = first_seg - 1000 * begun
    linked = jnp.where(seg_row == link_seg, F32(1.0), F32(0.0))
    in_last = jnp.where(seg_row == last_seg, F32(1.0), F32(0.0))
    linked_col = jnp.where(seg_col == link_seg, F32(1.0), F32(0.0))
    through = jnp.where(
        jnp.full((1, heads), link_seg, jnp.int32) == last_seg, F32(1.0), F32(0.0)
    )

    spot_t = lax.broadcasted_iota(jnp.int32, (rows, rows), 0)
    spot_s = lax.broadcasted_iota(jnp.int32, (rows, rows), 1)
    lower = spot_t >= spot_s
    causal = lower & (seg_col == seg_row)
    steps = jnp.transpose(step_ref[0])
    cumlog = lax.dot_general(
        jnp.where(lower, F32(1.0), F32(0.0)),
        -(steps * rate_ref[...]),
        (((1,), (0,)), ((), ())),
        precision=lax.Precision.HIGHEST,
        preferred_element_type=F32,
    )
    grown = jnp.exp(cumlog)
    shrunk = jnp.exp(-cumlog) * steps
    total = grown[rows - 1 : rows, :] * through
    tot_send[...] = jnp.zeros_like(tot_send)
    tot_send[:, :heads] = jnp.broadcast_to(total, (tot_send.shape[0], heads))

    tokens = tok_ref[0]
    both = jnp.concatenate([bw_ref[...], cw_ref[...]], axis=0)
    rounded = dot_nt(tokens, both).astype(BF16)
    turned = jnp.transpose(rounded.astype(F32))
    b_mat, c_mat = rounded[:, :states], rounded[:, states:]
    b_turned, c_turned = turned[:states, :], turned[states:, :]
    b_last = (b_turned * in_last).astype(BF16)
    c_open = (c_turned * linked).astype(BF16)
    c_linked = (c_mat.astype(F32) * linked_col).astype(BF16)

    def expander(at):
        head = lax.broadcasted_iota(jnp.int32, (heads, cut), 0)
        lane = lax.broadcasted_iota(jnp.int32, (heads, cut), 1) + at
        inside = (lane >= head * width) & (lane < head * width + width)
        return jnp.where(inside, F32(1.0), F32(0.0)).astype(BF16)

    sent_orders = [order_ref[0, (me + k) % n_seq] for k in range(1, n_seq)]
    got_orders = [order_ref[0, (me + n_seq - k) % n_seq] for k in range(1, n_seq)]
    pl.semaphore_wait(barrier, greeted)
    pieces = inner // cut

    def send(source, landing, ssem, rsem, k):
        copy = pltpu.make_async_remote_copy(
            src_ref=source,
            dst_ref=landing,
            send_sem=ssem,
            recv_sem=rsem,
            device_id=(dp, (me + k) % n_seq),
            device_id_type=MESH,
        )
        copy.start()
        return copy

    tot_copies = [
        send(tot_send, tot_recv.at[k - 1], tot_ssem.at[k - 1], tot_rsem.at[k - 1], k)
        for k in range(1, n_seq)
    ]
    sends = []
    for i in range(pieces):
        lanes = slice(i * cut, i * cut + cut)
        spreader = expander(i * cut)
        grown_x = spread(grown, spreader)
        ec_buf[:, lanes] = grown_x
        u_part = (x_ref[0, :, lanes].astype(F32) * spread(shrunk, spreader)).astype(BF16)
        v_part = (g_ref[0, :, lanes].astype(F32) * grown_x).astype(BF16)
        u_buf[:, lanes] = u_part
        v_buf[:, lanes] = v_part
        state = dot(b_last, u_part) * grown_x[rows - 1 : rows, :]
        adjoint = dot(c_open, v_part)
        group = []
        for k in range(1, n_seq):
            later = jnp.full(state.shape, sent_orders[k - 1], jnp.int32) > mine
            t_send[k - 1, i] = jnp.where(later, state, adjoint)
            slot = (k - 1) * pieces + i
            group.append(
                send(
                    t_send.at[k - 1, i],
                    t_recv.at[k - 1, i],
                    t_ssem.at[slot],
                    t_rsem.at[slot],
                    k,
                )
            )
        sends.append(group)

    scores = jnp.where(causal, dot_nt(c_mat, b_mat), F32(0.0)).astype(BF16)
    mixing = jnp.zeros((rows, rows), F32)
    for at in range(0, inner, cut):
        lanes = slice(at, at + cut)
        u_part = u_buf[:, lanes]
        yin_buf[:, lanes] = dot(scores, u_part)
        mixing = mixing + dot_nt(v_buf[:, lanes], u_part)
    mixing = jnp.where(causal, mixing, F32(0.0))
    mixing = mixing.astype(BF16)
    grad_c = dot_nt(b_turned.astype(BF16), mixing)
    grad_b = dot(c_turned.astype(BF16), mixing)

    for copy in tot_copies:
        copy.wait()

    weights = []
    for k in range(n_seq - 1):
        weight = jnp.ones((8, heads), F32)
        own = jnp.full((8, heads), got_orders[k], jnp.int32)
        low, high = jnp.minimum(own, mine), jnp.maximum(own, mine)
        for other in range(n_seq - 1):
            if other != k:
                inside = (low < got_orders[other]) & (got_orders[other] < high)
                weight = weight * jnp.where(inside, tot_recv[other, :, :heads], F32(1.0))
        weights.append(weight)
    skips = jnp.broadcast_to(skip_ref[...], (8, heads))
    cross_c = jnp.zeros((states, rows), F32)
    cross_b = jnp.zeros((states, rows), F32)
    for i in range(pieces):
        lanes = slice(i * cut, i * cut + cut)
        spreader = expander(i * cut)
        factors = [spread(weight, spreader)[:1, :] for weight in weights]
        incoming = jnp.zeros((states, cut), F32)
        returning = jnp.zeros((states, cut), F32)
        for copy in sends[i]:
            copy.wait()
        for k in range(n_seq - 1):
            term = t_recv[k, i] * factors[k]
            earlier = jnp.full(term.shape, got_orders[k], jnp.int32) < mine
            incoming = incoming + jnp.where(earlier, term, F32(0.0))
            returning = returning + jnp.where(earlier, F32(0.0), term)
        incoming = incoming.astype(BF16)
        in_buf[:, lanes] = incoming
        returning = (returning * ec_buf[rows - 1 : rows, lanes]).astype(BF16)
        cross_c = cross_c + dot_nt(incoming, v_buf[:, lanes])
        cross_b = cross_b + dot_nt(returning, u_buf[:, lanes])
    grad_c = (grad_c + cross_c * linked).astype(BF16)
    grad_b = (grad_b + cross_b * in_last).astype(BF16)
    grads = jnp.concatenate([grad_b, grad_c], axis=0)
    share = 2 * states // 8
    columns = depth // lane_cut
    for i in range(columns):
        block = dot(grads, tok_ref[0, :, i * lane_cut : (i + 1) * lane_cut])
        part[i * share : (i + 1) * share] = block.reshape(share, 8, lane_cut)
    for i in range(columns * share, part.shape[0]):
        part[i] = jnp.zeros((8, lane_cut), F32)

    def finish(i):
        lanes = slice(i * cut, i * cut + cut)
        y_part = yin_buf[:, lanes] + dot(c_linked, in_buf[:, lanes])
        y_part = ec_buf[:, lanes] * y_part
        skip_x = spread(skips, expander(i * cut))[:1, :]
        y_part = y_part + skip_x * x_ref[0, :, lanes].astype(F32)
        y_ref[0, :, lanes] = y_part.astype(BF16)

    undone = list(range(pieces))
    base = jnp.int32(0)
    extent = part.shape[0]
    owned = []
    used = 0
    for count, place, peer, landing in stages:
        extent = extent // count
        copies = []
        for k in range(1, count):
            theirs = base + ((place + k) % count) * extent
            copy = pltpu.make_async_remote_copy(
                src_ref=part.at[pl.ds(theirs, extent)],
                dst_ref=landing.at[k - 1],
                send_sem=rs_ssem.at[used],
                recv_sem=rs_rsem.at[used],
                device_id=peer(k),
                device_id_type=MESH,
            )
            copy.start()
            copies.append(copy)
            used += 1
        base = base + place * extent
        owned.append((base, extent))
        for i in undone[:2]:
            finish(i)
        undone = undone[2:]
        for copy in copies:
            copy.wait()
        summed = part[pl.ds(base, extent)]
        for k in range(len(copies)):
            summed = summed + landing[k]
        part[pl.ds(base, extent)] = summed
    whole[pl.ds(base, extent)] = part[pl.ds(base, extent)]
    for i in undone:
        finish(i)

    used = 0
    for (count, place, peer, _), (at, extent) in zip(stages[::-1], owned[::-1]):
        copies = []
        for k in range(1, count):
            copy = pltpu.make_async_remote_copy(
                src_ref=whole.at[pl.ds(at, extent)],
                dst_ref=whole.at[pl.ds(at, extent)],
                send_sem=ag_ssem.at[used],
                recv_sem=ag_rsem.at[used],
                device_id=peer(k),
                device_id_type=MESH,
            )
            copy.start()
            copies.append(copy)
            used += 1
        for copy in copies:
            copy.wait()
    for i in range(columns):
        block = whole[i * share : (i + 1) * share].reshape(2 * states, lane_cut)
        gb_ref[:, i * lane_cut : (i + 1) * lane_cut] = block[:states]
        gc_ref[:, i * lane_cut : (i + 1) * lane_cut] = block[states:]


def per_device(
    layer_in,
    scan_in,
    step_size,
    b_weight,
    c_weight,
    decay_rate,
    skip_gain,
    out_grad,
    doc_lengths,
    block_order,
):
    n_dp, n_seq = lax.axis_size("dp"), lax.axis_size("seq")
    rows, inner = scan_in.shape[1], scan_in.shape[2]
    depth, states = b_weight.shape
    cores, nz, nx, ny = plan(n_dp, n_seq)
    devices = n_dp * n_seq
    units = depth // 128 * (2 * states // 8)
    padded = devices * (-(-units // devices))
    landings = []
    extent = padded
    for count in (cores, nx, ny, nz):
        extent = extent // count
        landings.append(pltpu.VMEM((max(count - 1, 1), extent, 8, 128), F32))
    hops = max(cores + nx + ny + nz - 4, 1)
    links = max(n_seq - 1, 1)
    cut = 512 if inner % 512 == 0 else inner
    pieces = inner // cut
    vmem = pl.BlockSpec(memory_space=pltpu.VMEM)
    smem = pl.BlockSpec(memory_space=pltpu.SMEM)
    dma = pltpu.SemaphoreType.DMA
    scan_out, b_sum, c_sum = pl.pallas_call(
        functools.partial(kernel, n_dp, n_seq, depth),
        out_shape=(
            jax.ShapeDtypeStruct((1, rows, inner), BF16),
            jax.ShapeDtypeStruct((states, depth), F32),
            jax.ShapeDtypeStruct((states, depth), F32),
        ),
        in_specs=[vmem] * 8 + [smem] * 2,
        out_specs=(vmem, vmem, vmem),
        scratch_shapes=[
            pltpu.VMEM((rows, inner), BF16),
            pltpu.VMEM((rows, inner), BF16),
            pltpu.VMEM((rows, inner), F32),
            pltpu.VMEM((rows, inner), F32),
            pltpu.VMEM((states, inner), BF16),
            pltpu.VMEM((links, pieces, states, cut), F32),
            pltpu.VMEM((links, pieces, states, cut), F32),
            pltpu.VMEM((8, 128), F32),
            pltpu.VMEM((links, 8, 128), F32),
            pltpu.VMEM((padded, 8, 128), F32),
            pltpu.VMEM((padded, 8, 128), F32),
            *landings,
            dma((links * pieces,)),
            dma((links * pieces,)),
            dma((links,)),
            dma((links,)),
            dma((hops,)),
            dma((hops,)),
            dma((hops,)),
            dma((hops,)),
        ],
        compiler_params=pltpu.CompilerParams(
            collective_id=0, has_side_effects=True, vmem_limit_bytes=60 * 1024 * 1024
        ),
    )(
        layer_in,
        scan_in,
        jnp.swapaxes(step_size, 1, 2),
        b_weight.T,
        c_weight.T,
        decay_rate[None, :],
        skip_gain[None, :],
        out_grad,
        doc_lengths,
        block_order,
    )
    scale = 1.0 / (n_dp * n_seq * rows)
    return (scan_out, (b_sum * scale).T, (c_sum * scale).T)


def solution(mesh):
    blocks = P("dp", "seq", None)
    in_specs = (blocks, blocks, blocks, P(), P(), P(), P(), blocks, P("dp", None), P("dp", None))
    return jax.shard_map(
        per_device, mesh=mesh, in_specs=in_specs, out_specs=(blocks, P(), P()), check_vma=False
    )
```
